128 devices in a mesh: dev: 128 (over z, x, y, core).
Axes of the slice: x: 4, y: 4, z: 4, core: 2. Of those that a mesh axis runs over, the one named last changes fastest.
Arguments:
- occurrence: bfloat16 [8192, 128, 128], P('dev'), may hold values from -0.5 to 0.5
- block_owner: int32 [8192, 1], P('dev'), may hold values from 0 to 127; in each aligned block of 64 rows (0 to 63, 64 to 127, ...) no two rows name the same one
- read_block: int32 [8192], P('dev'), may hold values from 0 to 15
- slot_order: int32 [128, 128], P('dev'), may hold values from 0 to 127, each once within a row
Outputs:
- margin: float32 [262144, 512], P('dev')
The draws below stay inside these ranges and needn't reach their ends.
Inputs may be any that keep to these rules, and one draw needn't show every extreme that they name: `block_owner`: among the blocks of one device no owner is named more than 1 times, a bound that some block reaches. `slot_order`: each row names every number of 0 to 127 once.
All inputs are finite; a program needn't handle non-finite values.
Results may differ from the reference program's by a relative error of at most 0.0026.
Values may be sent and summed in bfloat16 or wider, within the bound.
No kernel may reach another device: no remote copies, remote signals or barrier semaphores. Data moves between devices by JAX's collectives and lax.ppermute only.
A program may use at most 128 MiB of HBM per device.

```python
import math
import jax
import jax.numpy as jnp
import numpy as np
from jax import lax

RB = 128
KB = 128
CAP = 4
S_DEV = 64
RB_DEV = 16
PAIR_MOST = 1
BLOCKS = 8192
N_DEV = 128


def with_ends(array, stream_key, smallest, high):
    longest = array.shape.index(max(array.shape))
    spots = []
    for shift in (0, 1):
        where = [jax.random.randint(jax.random.fold_in(stream_key, axis), (), 0, length) for axis, length in enumerate(array.shape)]
        where[longest] = (where[longest] + shift) % array.shape[longest]
        spots.append(tuple(where))
    return array.at[spots[0]].set(smallest).at[spots[1]].set(high)


def level_of(own_key, dims, shards, smallest, high):
    gain, own = 1.0, jax.random.fold_in(own_key, 6)
    for axis_at, blocks in shards:
        heights = jnp.exp(jax.random.uniform(jax.random.fold_in(own, axis_at), (blocks,), jnp.float32, smallest / len(shards), high / len(shards)))
        gain = gain * jnp.repeat(heights, dims[axis_at] // blocks).reshape([-1 if axis == axis_at else 1 for axis in range(len(dims))])
    return gain


def shared_out(rng, own, number, rows, count, top, reach, lean):
    sequence = jax.random.permutation(rng, count)
    heavy_load, usual = shares(count, rows * top, reach, lean, True), shares(count, rows * top, reach, lean, False)
    places = jnp.arange(count)

    def named(sizes, turn):
        used = int((sizes > 0).sum())
        fixed = max(1, used // 4)
        moved = fixed + (places - fixed + turn * (used - fixed)) % max(1, count - fixed)
        return jnp.zeros((count,), jnp.int32).at[sequence[jnp.where(places < fixed, places, moved)]].set(jnp.asarray(sizes, jnp.int32))

    sizes = jnp.where(number % 4 == 0, named(heavy_load, number // 4), named(usual, number - number // 4 - 1))
    mixed = jax.random.permutation(jax.random.fold_in(own, 3), count)
    giver, taker = mixed[0:count // 2 * 2:2], mixed[1:count // 2 * 2:2]
    margin = jnp.minimum(sizes[giver] - 1, reach - sizes[taker]) // 2
    margin = jnp.where((giver == sequence[0]) | (taker == sequence[0]) | (sizes[taker] == 0), 0, jnp.maximum(margin, 0))
    moved = jax.random.randint(jax.random.fold_in(own, 4), (count // 2,), 0, 1 << 20) % (margin + 1)
    sizes = sizes.at[giver].add(-moved).at[taker].add(moved)
    labels = jnp.searchsorted(jnp.cumsum(sizes), jnp.arange(rows * top), side="right").astype(jnp.int32)
    table = labels.reshape(top, rows).T
    table = table[jax.random.permutation(jax.random.fold_in(own, 1), rows)]
    turn = jax.random.randint(jax.random.fold_in(own, 2), (rows, 1), 0, top)
    return jnp.take_along_axis(table, (jnp.arange(top)[None, :] + turn) % top, axis=1)


def shares(number_of, total, limit, lean, full):
    portions = [(1 << 20) // math.isqrt(grade ** lean) + 1 for grade in range(1, number_of + 1)]
    largest = limit if full else min(limit, max(-(-total // number_of), total * portions[0] // sum(portions)))
    least = 1 if total - largest >= number_of - 1 else 0
    counts, spare = [largest] + [least] * (number_of - 1), total - largest - least * (number_of - 1)
    while spare > 0:
        candidates = [i for i in range(1, number_of) if counts[i] < largest] or [i for i in range(1, number_of) if counts[i] < limit]
        whole, budget = sum([portions[i] for i in candidates]), spare
        for i in candidates:
            addition = min(limit - counts[i], max(1, budget * portions[i] // whole), spare)
            counts[i] = counts[i] + addition
            spare = spare - addition
    return np.array(counts)


def noise(key, extent, scale, reach, shards=(), held_as=jnp.bfloat16):
    loudness = level_of(key, extent, shards, -0.22, 0.18) if shards else 1.0
    drawn = jax.random.normal(key, extent, jnp.float32) * scale * loudness
    return jnp.minimum(jnp.maximum(drawn, -reach), reach).astype(held_as)


def setup_inputs(seed: int = 0) -> dict:
    arg_keys = jax.random.split(jax.random.key(seed), 5)
    occurrence = noise(arg_keys[0], (BLOCKS, RB, KB), KB ** -0.5, 0.5, ((0, 128),))
    block_owner_keys = jax.random.split(jax.random.fold_in(arg_keys[1], 1), BLOCKS // S_DEV)
    block_owner_turns = jax.random.permutation(jax.random.fold_in(arg_keys[1], 3), BLOCKS // S_DEV)
    block_owner = jax.vmap(lambda own, number: shared_out(jax.random.fold_in(arg_keys[1], 2), own, number, S_DEV, N_DEV, 1, PAIR_MOST, 2))(block_owner_keys, block_owner_turns).reshape((BLOCKS, 1))
    read_block = with_ends(jax.random.randint(arg_keys[2], (BLOCKS,), 0, RB_DEV), jax.random.fold_in(arg_keys[2], 1), 0, RB_DEV - 1).astype(jnp.int32)
    slot_order = jax.vmap(lambda own: jax.random.permutation(own, N_DEV * PAIR_MOST))(jax.random.split(arg_keys[3], N_DEV)).reshape((N_DEV, N_DEV * PAIR_MOST)).astype(jnp.int32)
    return dict(occurrence=occurrence, block_owner=block_owner, read_block=read_block, slot_order=slot_order)


def reference(occurrence, block_owner, read_block, slot_order):
    block_total = occurrence.shape[0]
    slot_total = N_DEV * PAIR_MOST
    owners = block_owner[:, 0].reshape(N_DEV, S_DEV)
    positions = jnp.arange(S_DEV, dtype=jnp.int32)
    earlier = positions[None, :] < positions[:, None]
    same_owner = owners[:, :, None] == owners[:, None, :]
    earlier_count = jnp.sum((same_owner & earlier[None]).astype(jnp.int32), axis=2).astype(jnp.int32)
    source = jnp.arange(N_DEV, dtype=jnp.int32)[:, None]
    slot_index = (source * PAIR_MOST + earlier_count).astype(jnp.int32)
    holder = jnp.full((N_DEV, slot_total), -1, jnp.int32)
    holder = holder.at[owners.reshape(-1), slot_index.reshape(-1)].set(jnp.arange(block_total, dtype=jnp.int32))
    ordered_holder = jnp.take_along_axis(holder, slot_order.astype(jnp.int32), axis=1)
    holder_safe = jnp.maximum(ordered_holder, 0)
    stacked = jnp.where((ordered_holder >= 0)[:, :, None, None], occurrence[holder_safe], jnp.zeros((), occurrence.dtype))
    groups = stacked.reshape(N_DEV, slot_total // CAP, CAP, RB, KB)
    owner_rows = jnp.arange(N_DEV, dtype=jnp.int32)[:, None] + jnp.zeros((1, slot_total), jnp.int32)
    place_of = jnp.zeros((N_DEV, slot_total), jnp.int32)
    place_of = place_of.at[owner_rows, slot_order.astype(jnp.int32)].set(
        jnp.zeros((N_DEV, 1), jnp.int32) + jnp.arange(slot_total, dtype=jnp.int32)[None, :])
    by_source = occurrence.reshape(N_DEV, S_DEV, RB, KB)
    read_rows = read_block.reshape(N_DEV, S_DEV)

    def one_source(carried, source_index):
        own_blocks = by_source[source_index]
        own_owner = owners[source_index]
        own_place = place_of[own_owner, slot_index[source_index]]
        group_blocks = groups[own_owner, own_place // CAP]
        tile_block = jnp.einsum('bik,bjrk->bijr', own_blocks.astype(jnp.float32), group_blocks.astype(jnp.float32))
        tile_block = tile_block.astype(jnp.bfloat16)
        onehot = (read_rows[source_index][None, :] == jnp.arange(RB_DEV, dtype=jnp.int32)[:, None]).astype(jnp.float32)
        summed = jnp.einsum('nb,bijr->nijr', onehot, tile_block.astype(jnp.float32))
        return carried, summed.reshape(RB_DEV * RB, CAP * RB)

    _, per_source = lax.scan(one_source, jnp.zeros((), jnp.float32), jnp.arange(N_DEV, dtype=jnp.int32))
    return per_source.reshape(N_DEV * RB_DEV * RB, CAP * RB)
```

```python
import jax
import jax.numpy as jnp
from jax import lax
from jax.experimental import pallas as pl
from jax.experimental.pallas import tpu as pltpu
from jax.sharding import PartitionSpec as P

CAP = 4
RB_DEV = 16
LIST = 256
ROOMS = (128, 144)
CHUNK = 16


def lists_kernel(me_ref, read_ref, shared_ref, list_ref, plan_ref, most_ref, order_ref, owner_ref, rank_ref, value_ref):
    f32, bf16 = jnp.float32, jnp.bfloat16
    devices = shared_ref.shape[0]
    blocks = read_ref.shape[1]
    square = (devices, devices)
    most = (CAP - 1) * blocks

    def iota(shape, axis):
        return lax.broadcasted_iota(jnp.int32, shape, axis).astype(f32)

    order = shared_ref[:, :devices]
    order_ref[...] = order.astype(f32).T
    owner_ref[...] = shared_ref[:, devices : 2 * devices].astype(f32).T
    row, lane = iota(square, 0), iota(square, 1)

    def hold(n, held):
        return jnp.where(owner_ref[pl.ds(n, 1), :] == row, (n + 1).astype(f32), held)

    def stand(q, place):
        return jnp.where(order_ref[pl.ds(q, 1), :] == row, q.astype(f32), place)

    held = lax.fori_loop(0, blocks, hold, jnp.zeros(square, f32))
    place = lax.fori_loop(0, devices, stand, jnp.zeros(square, f32)).T.astype(jnp.int32)
    there = jnp.take_along_axis(held, order, axis=1)
    number = jnp.where(there > 0.0, order.astype(f32) * blocks + there, 0.0)
    values = [
        jnp.where(held > 0.0, jnp.take_along_axis(number, place ^ j, axis=1), 0.0)
        for j in range(1, CAP)
    ]
    needs = [(v > 0.0).astype(f32) for v in values]
    total = needs[0] + needs[1] + needs[2]
    below = (lane < row).astype(f32).astype(bf16)
    rank = jnp.dot(below, total.astype(bf16), preferred_element_type=f32)
    ranks = []
    for j in range(CAP - 1):
        ranks.append(jnp.where(needs[j] > 0.0, rank, -1.0))
        rank = rank + needs[j]
        rank_ref[j] = ranks[j]
        value_ref[j] = values[j] - 1.0
    count = jnp.max(rank[devices - 1 :, :])
    most_ref[0] = sum((count > room).astype(jnp.int32) for room in ROOMS)
    turn = iota((most, devices), 0)

    def fill(o, found):
        for j in range(CAP - 1):
            hit = rank_ref[j, pl.ds(o, 1), :] == turn
            found = jnp.where(hit, value_ref[j, pl.ds(o, 1), :], found)
        return found

    found = lax.fori_loop(0, devices, fill, jnp.zeros((most, devices), f32))
    list_ref[:, :devices] = found[:devices].T.astype(jnp.int32)
    rest = jnp.concatenate([found[devices:], jnp.zeros((LIST - most, devices), f32)], axis=0)
    list_ref[:, devices:] = rest.T.astype(jnp.int32)

    me = me_ref[0].astype(f32)

    def mine(array):
        return jnp.sum(jnp.where(lane == me, array, 0.0), axis=1, keepdims=True)

    reads = read_ref[...].astype(f32)
    row, column = iota((blocks, blocks), 0), iota((blocks, blocks), 1)
    read = jnp.sum(jnp.where(row == column, reads, 0.0), axis=1, keepdims=True)
    before = (read < reads) | ((read == reads) & (row < column))
    at = jnp.sum(before.astype(f32), axis=0, keepdims=True)
    own = mine(held)
    chosen = own == iota((devices, blocks), 1) + 1.0
    at = jnp.sum(jnp.where(chosen, at, 0.0), axis=1, keepdims=True)
    read = jnp.sum(jnp.where(chosen, reads, 0.0), axis=1, keepdims=True)
    turn = (at == lane) & (own > 0.0)
    stands = mine((place & (CAP - 1)).astype(f32))
    spots = [-1.0 - own] + [mine(r) for r in ranks]
    rows = []
    for j in range(CAP):
        spot = jnp.zeros_like(own)
        for p in range(CAP):
            spot = jnp.where(stands == float(p), spots[p ^ j], spot)
        rows.append(jnp.sum(jnp.where(turn, spot, 0.0), axis=0, keepdims=True))
    rows.append(jnp.sum(jnp.where(turn, own - 1.0, 0.0), axis=0, keepdims=True))
    by_read = jnp.sum(jnp.where(turn, read, 0.0), axis=0, keepdims=True)
    rows.append(jnp.where(iota((1, devices), 1) < blocks, by_read, float(RB_DEV)))
    rows += [jnp.zeros((1, devices), f32)] * 2
    plan_ref[...] = jnp.concatenate(rows, axis=0).astype(jnp.int32)


def lists(me, read, shared):
    devices = shared.shape[0]
    whole = pl.BlockSpec(memory_space=pltpu.VMEM)
    small = pl.BlockSpec(memory_space=pltpu.SMEM)
    return pl.pallas_call(
        lists_kernel,
        in_specs=[small, whole, whole],
        out_specs=(whole, whole, small),
        out_shape=(
            jax.ShapeDtypeStruct((devices, LIST), jnp.int32),
            jax.ShapeDtypeStruct((8, devices), jnp.int32),
            jax.ShapeDtypeStruct((1,), jnp.int32),
        ),
        scratch_shapes=[
            pltpu.VMEM((devices, devices), jnp.float32),
            pltpu.VMEM((devices, devices), jnp.float32),
            pltpu.VMEM((CAP - 1, devices, devices), jnp.float32),
            pltpu.VMEM((CAP - 1, devices, devices), jnp.float32),
        ],
        name="lists",
    )(me, read, shared)


def pick_kernel(list_ref, rows_ref, out_ref, wide_ref, stage_ref):
    group, room, _ = out_ref.shape
    step = pl.program_id(0)

    @pl.when(step == 0)
    def _():
        wide_ref[...] = rows_ref[...].astype(jnp.float32)

    for i in range(group):
        base = (step * group + i) * LIST
        stage = stage_ref.at[i % 2]
        for t in range(room):
            stage[pl.ds(t, 1), :] = wide_ref[pl.ds(list_ref[base + t], 1), :]
        out_ref[i] = stage[...].astype(out_ref.dtype)


def pick_rows(listed, rows, room):
    total, lanes = rows.shape
    devices, group = listed.shape[0] // LIST, 4
    return pl.pallas_call(
        pick_kernel,
        grid=(devices // group,),
        in_specs=[
            pl.BlockSpec(memory_space=pltpu.SMEM),
            pl.BlockSpec((total, lanes), lambda i: (0, 0), pipeline_mode=pl.Buffered(1)),
        ],
        out_specs=pl.BlockSpec((group, room, lanes), lambda i: (i, 0, 0)),
        out_shape=jax.ShapeDtypeStruct((devices, room, lanes), rows.dtype),
        scratch_shapes=[
            pltpu.VMEM((total, lanes), jnp.float32),
            pltpu.VMEM((2, room, lanes), jnp.float32),
        ],
        name="pick_rows",
    )(listed, rows)


def margin_kernel(plan_ref, own_ref, got_ref, out_ref, in_ref, wide_ref, block_ref, sum_ref, in_sem, out_sem):
    rows, room, lanes = got_ref.shape
    blocks = own_ref.shape[0]
    f32, bf16 = jnp.float32, jnp.bfloat16
    chunks = room // CHUNK
    copies = [
        pltpu.make_async_copy(
            got_ref.at[:, pl.ds(c * CHUNK, CHUNK), :], in_ref.at[c], in_sem.at[c]
        )
        for c in range(chunks)
    ]
    for copy in copies:
        copy.start()
    sum_ref[...] = jnp.zeros(sum_ref.shape, f32)
    block_ref[room] = jnp.zeros((rows, lanes), bf16)
    for b in range(blocks):
        block_ref[room + 1 + b] = own_ref[b]
    for c, copy in enumerate(copies):
        copy.wait()
        wide = wide_ref.at[c % 2]
        wide[...] = in_ref[c].astype(f32).reshape(rows * CHUNK, lanes)
        for t in range(CHUNK):
            block_ref[c * CHUNK + t] = wide[pl.ds(t, rows, stride=CHUNK), :].astype(bf16)

    def send(r):
        part = pl.ds(pl.multiple_of(r * rows, rows), rows)
        return pltpu.make_async_copy(sum_ref.at[part], out_ref.at[part], out_sem)

    def tiles(i):
        own = own_ref[plan_ref[CAP, i]]
        for j in range(CAP):
            spot = plan_ref[j, i]
            spot = jnp.where(spot < 0, room - 1 - spot, spot)
            yield lax.dot_general(
                own, block_ref[spot], (((1,), (1,)), ((), ())), preferred_element_type=f32
            ).astype(bf16).astype(f32)

    unroll = 2

    def step(q, carry):
        at = [q * unroll + u for u in range(unroll)]
        found = [list(tiles(i)) for i in at]
        for i, tile in zip(at, found):
            part = pl.ds(pl.multiple_of(plan_ref[CAP + 1, i] * rows, rows), rows)
            for j in range(CAP):
                sum_ref[part, j * rows : (j + 1) * rows] += tile[j]
        start = jnp.where(q == 0, 0, plan_ref[CAP + 1, at[0]])

        def leave(r, carry):
            send(r).start()
            return carry

        lax.fori_loop(start, plan_ref[CAP + 1, at[-1] + 1], leave, 0)
        return carry

    lax.fori_loop(0, blocks // unroll, step, 0)
    pltpu.make_async_copy(sum_ref, out_ref, out_sem).wait()


def margins(plan, own, got):
    rows, room, lanes = got.shape
    blocks = own.shape[0]
    return pl.pallas_call(
        margin_kernel,
        in_specs=[
            pl.BlockSpec(memory_space=pltpu.SMEM),
            pl.BlockSpec(memory_space=pltpu.VMEM),
            pl.BlockSpec(memory_space=pl.ANY),
        ],
        out_specs=pl.BlockSpec(memory_space=pl.ANY),
        out_shape=jax.ShapeDtypeStruct((RB_DEV * rows, CAP * rows), jnp.float32),
        scratch_shapes=[
            pltpu.VMEM((room // CHUNK, rows, CHUNK, lanes), got.dtype),
            pltpu.VMEM((2, rows * CHUNK, lanes), jnp.float32),
            pltpu.VMEM((room + 1 + blocks, rows, lanes), own.dtype),
            pltpu.VMEM((RB_DEV * rows, CAP * rows), jnp.float32),
            pltpu.SemaphoreType.DMA((room // CHUNK,)),
            pltpu.SemaphoreType.DMA,
        ],
        name="margins",
    )(plan, own, got)


def exchange(array):
    return lax.all_to_all(array, "dev", split_axis=0, concat_axis=0, tiled=True)


def shards(occurrence, block_owner, read_block, slot_order):
    devices = lax.axis_size("dev")
    blocks, _, kmers = occurrence.shape
    owner, read = block_owner.reshape(1, blocks), read_block.reshape(1, blocks)
    held_rows = exchange(occurrence.transpose(1, 0, 2))
    held_rows = held_rows.reshape(devices * blocks, kmers)
    own_row = jnp.concatenate(
        [slot_order, owner, jnp.zeros((1, devices - blocks), jnp.int32)], axis=1
    )
    shared = exchange(jnp.broadcast_to(own_row[:, None], (devices, 1, 2 * devices)))
    me = lax.axis_index("dev").astype(jnp.int32).reshape(1)
    listed, plan, branch = lists(me, read, shared.reshape(devices, 2 * devices))
    listed = listed.reshape(devices * LIST)

    def finish(room):
        outgoing = pick_rows(listed, held_rows, room)
        return margins(plan, occurrence, exchange(outgoing))

    rooms = ROOMS + ((CAP - 1) * blocks,)
    return lax.switch(branch[0], [lambda room=room: finish(room) for room in rooms])


def solution(mesh):
    placed = (P("dev", None, None), P("dev", None), P("dev"), P("dev", None))

    return jax.shard_map(
        shards, mesh=mesh, in_specs=placed, out_specs=P("dev", None), check_vma=False
    )
```

```python
import jax
import jax.numpy as jnp
from jax import lax
from jax.experimental import pallas as pl
from jax.experimental.pallas import tpu as pltpu
from jax.sharding import PartitionSpec as P

CAP = 4
RB_DEV = 16
ROOMS = (128, 144)
CHUNK = 16


def lists_kernel(me_ref, read_ref, shared_ref, list_ref, plan_ref, most_ref, order_ref, owner_ref, rank_ref, value_ref):
    f32, bf16 = jnp.float32, jnp.bfloat16
    devices = shared_ref.shape[0]
    blocks = read_ref.shape[1]
    square = (devices, devices)
    most = (CAP - 1) * blocks

    def iota(shape, axis):
        return lax.broadcasted_iota(jnp.int32, shape, axis).astype(f32)

    order = shared_ref[:, :devices]
    order_ref[...] = order.astype(f32).T
    owner_ref[...] = shared_ref[:, devices : 2 * devices].astype(f32).T
    row, lane = iota(square, 0), iota(square, 1)

    def hold(n, held):
        return jnp.where(owner_ref[pl.ds(n, 1), :] == row, (n + 1).astype(f32), held)

    def stand(q, place):
        return jnp.where(order_ref[pl.ds(q, 1), :] == row, q.astype(f32), place)

    held = lax.fori_loop(0, blocks, hold, jnp.zeros(square, f32))
    place = lax.fori_loop(0, devices, stand, jnp.zeros(square, f32)).T.astype(jnp.int32)
    there = jnp.take_along_axis(held, order, axis=1)
    number = jnp.where(there > 0.0, order.astype(f32) * blocks + there, 0.0)
    values = [
        jnp.where(held > 0.0, jnp.take_along_axis(number, place ^ j, axis=1), 0.0)
        for j in range(1, CAP)
    ]
    needs = [(v > 0.0).astype(f32) for v in values]
    total = needs[0] + needs[1] + needs[2]
    below = (lane < row).astype(f32).astype(bf16)
    rank = jnp.dot(below, total.astype(bf16), preferred_element_type=f32)
    ranks = []
    for j in range(CAP - 1):
        ranks.append(jnp.where(needs[j] > 0.0, rank, -1.0))
        rank = rank + needs[j]
        rank_ref[j] = ranks[j]
        value_ref[j] = values[j] - 1.0
    count = jnp.max(rank[devices - 1 :, :])
    most_ref[0] = sum((count > room).astype(jnp.int32) for room in ROOMS)
    turn = iota((most, devices), 0)

    def fill(o, found):
        for j in range(CAP - 1):
            hit = rank_ref[j, pl.ds(o, 1), :] == turn
            found = jnp.where(hit, value_ref[j, pl.ds(o, 1), :], found)
        return found

    found = lax.fori_loop(0, devices, fill, jnp.zeros((most, devices), f32))
    list_ref[:, 0, :] = found.astype(jnp.int32)

    me = me_ref[0].astype(f32)

    def mine(array):
        return jnp.sum(jnp.where(lane == me, array, 0.0), axis=1, keepdims=True)

    reads = read_ref[...].astype(f32)
    row, column = iota((blocks, blocks), 0), iota((blocks, blocks), 1)
    read = jnp.sum(jnp.where(row == column, reads, 0.0), axis=1, keepdims=True)
    before = (read < reads) | ((read == reads) & (row < column))
    at = jnp.sum(before.astype(f32), axis=0, keepdims=True)
    own = mine(held)
    chosen = own == iota((devices, blocks), 1) + 1.0
    at = jnp.sum(jnp.where(chosen, at, 0.0), axis=1, keepdims=True)
    read = jnp.sum(jnp.where(chosen, reads, 0.0), axis=1, keepdims=True)
    turn = (at == lane) & (own > 0.0)
    stands = mine((place & (CAP - 1)).astype(f32))
    spots = [-1.0 - own] + [mine(r) for r in ranks]
    rows = []
    for j in range(CAP):
        spot = jnp.zeros_like(own)
        for p in range(CAP):
            spot = jnp.where(stands == float(p), spots[p ^ j], spot)
        rows.append(jnp.sum(jnp.where(turn, spot, 0.0), axis=0, keepdims=True))
    rows.append(jnp.sum(jnp.where(turn, own - 1.0, 0.0), axis=0, keepdims=True))
    by_read = jnp.sum(jnp.where(turn, read, 0.0), axis=0, keepdims=True)
    rows.append(jnp.where(iota((1, devices), 1) < blocks, by_read, float(RB_DEV)))
    rows += [jnp.zeros((1, devices), f32)] * 2
    plan_ref[...] = jnp.concatenate(rows, axis=0).astype(jnp.int32)


def lists(me, read, shared):
    devices = shared.shape[0]
    whole = pl.BlockSpec(memory_space=pltpu.VMEM)
    small = pl.BlockSpec(memory_space=pltpu.SMEM)
    return pl.pallas_call(
        lists_kernel,
        in_specs=[small, whole, whole],
        out_specs=(whole, whole, small),
        out_shape=(
            jax.ShapeDtypeStruct(((CAP - 1) * read.shape[1], 1, devices), jnp.int32),
            jax.ShapeDtypeStruct((8, devices), jnp.int32),
            jax.ShapeDtypeStruct((1,), jnp.int32),
        ),
        scratch_shapes=[
            pltpu.VMEM((devices, devices), jnp.float32),
            pltpu.VMEM((devices, devices), jnp.float32),
            pltpu.VMEM((CAP - 1, devices, devices), jnp.float32),
            pltpu.VMEM((CAP - 1, devices, devices), jnp.float32),
        ],
        name="lists",
    )(me, read, shared)


def pick_kernel(list_ref, rows_ref, out_ref, wide_ref, stage_ref, spare_ref, list_sem, *asked):
    group, room, _ = out_ref.shape
    pairs = stage_ref.shape[0]

    @pl.when(pl.program_id(0) == 0)
    def _():
        copies = [
            pltpu.make_async_copy(list_ref.at[t], asked[t], list_sem) for t in range(room)
        ]
        for copy in copies:
            copy.start()
        wide_ref[...] = rows_ref[...].astype(jnp.float32)
        pltpu.make_async_copy(list_ref.at[pl.ds(0, room)], spare_ref, list_sem).wait()

    first = pl.program_id(0) * group

    def pick(i, carry):
        for u in range(pairs):
            at = i * pairs + u
            s = first + at
            for t in range(room):
                stage_ref[u, pl.ds(t, 1), :] = wide_ref[pl.ds(asked[t][0, s], 1), :]
            out_ref[at] = stage_ref[u].astype(out_ref.dtype)
        return carry

    lax.fori_loop(0, group // pairs, pick, 0)


def pick_rows(listed, rows, room):
    total, lanes = rows.shape
    devices, group, pairs = listed.shape[2], 8, 2
    return pl.pallas_call(
        pick_kernel,
        grid=(devices // group,),
        in_specs=[
            pl.BlockSpec(memory_space=pltpu.VMEM),
            pl.BlockSpec(memory_space=pltpu.VMEM),
        ],
        out_specs=pl.BlockSpec((group, room, lanes), lambda i: (i, 0, 0)),
        out_shape=jax.ShapeDtypeStruct((devices, room, lanes), rows.dtype),
        scratch_shapes=[
            pltpu.VMEM((total, lanes), jnp.float32),
            pltpu.VMEM((pairs, room, lanes), jnp.float32),
            pltpu.SMEM((room, 1, devices), jnp.int32),
            pltpu.SemaphoreType.DMA,
        ]
        + [pltpu.SMEM((1, devices), jnp.int32)] * room,
        name="pick_rows",
    )(listed, rows)


def margin_kernel(plan_ref, own_ref, got_ref, out_ref, in_ref, wide_ref, block_ref, sum_ref, other_ref, in_sem, out_sem):
    rows, room, lanes = got_ref.shape
    blocks = own_ref.shape[0]
    f32, bf16 = jnp.float32, jnp.bfloat16
    chunks = room // CHUNK
    apart = CHUNK + 1

    def fetch(c):
        return pltpu.make_async_copy(
            got_ref.at[:, pl.ds(pl.multiple_of(c * CHUNK, CHUNK), CHUNK), :], in_ref.at[c], in_sem.at[c]
        )

    for c in range(chunks):
        fetch(c).start()
    sum_ref[...] = jnp.zeros(sum_ref.shape, f32)
    other_ref[...] = jnp.zeros(other_ref.shape, f32)
    block_ref[room] = jnp.zeros((rows, lanes), bf16)

    def keep(b, carry):
        block_ref[room + 1 + b] = own_ref[b]
        return carry

    lax.fori_loop(0, blocks, keep, 0, unroll=8)

    def turn(c, carry):
        fetch(c).wait()

        def widen(d, carry):
            wide_ref[pl.ds(d * apart, CHUNK), :] = in_ref[c, d].astype(f32)
            return carry

        lax.fori_loop(0, rows, widen, 0, unroll=16)
        for t in range(CHUNK):
            block_ref[c * CHUNK + t] = wide_ref[pl.ds(t, rows, stride=apart), :].astype(bf16)
        return carry

    lax.fori_loop(0, chunks, turn, 0)

    def tiles(i):
        own = own_ref[plan_ref[CAP, i]]
        for j in range(CAP):
            spot = plan_ref[j, i]
            spot = jnp.where(spot < 0, room - 1 - spot, spot)
            yield lax.dot_general(
                own, block_ref[spot], (((1,), (1,)), ((), ())), preferred_element_type=f32
            ).astype(bf16).astype(f32)

    sums = (sum_ref, other_ref)
    unroll = 4

    def step(q, carry):
        for u in range(unroll):
            i = q * unroll + u
            part = pl.ds(pl.multiple_of(plan_ref[CAP + 1, i] * rows, rows), rows)
            for j, tile in enumerate(tiles(i)):
                sums[u % 2][part, j * rows : (j + 1) * rows] += tile
        return carry

    lax.fori_loop(0, blocks // unroll, step, 0)

    def leave(r, carry):
        part = pl.ds(pl.multiple_of(r * rows, rows), rows)
        sum_ref[part] += other_ref[part]
        pltpu.make_async_copy(sum_ref.at[part], out_ref.at[part], out_sem).start()
        return carry

    lax.fori_loop(0, RB_DEV, leave, 0)
    pltpu.make_async_copy(sum_ref, out_ref, out_sem).wait()


def margins(plan, own, got):
    rows, room, lanes = got.shape
    blocks = own.shape[0]
    return pl.pallas_call(
        margin_kernel,
        in_specs=[
            pl.BlockSpec(memory_space=pltpu.SMEM),
            pl.BlockSpec(memory_space=pltpu.VMEM),
            pl.BlockSpec(memory_space=pl.ANY),
        ],
        out_specs=pl.BlockSpec(memory_space=pl.ANY),
        out_shape=jax.ShapeDtypeStruct((RB_DEV * rows, CAP * rows), jnp.float32),
        scratch_shapes=[
            pltpu.VMEM((room // CHUNK, rows, CHUNK, lanes), got.dtype),
            pltpu.VMEM((rows * (CHUNK + 1), lanes), jnp.float32),
            pltpu.VMEM((room + 1 + blocks, rows, lanes), own.dtype),
            pltpu.VMEM((RB_DEV * rows, CAP * rows), jnp.float32),
            pltpu.VMEM((RB_DEV * rows, CAP * rows), jnp.float32),
            pltpu.SemaphoreType.DMA((room // CHUNK,)),
            pltpu.SemaphoreType.DMA,
        ],
        name="margins",
    )(plan, own, got)


def exchange(array):
    return lax.all_to_all(array, "dev", split_axis=0, concat_axis=0, tiled=True)


def shards(occurrence, block_owner, read_block, slot_order):
    devices = lax.axis_size("dev")
    blocks, _, kmers = occurrence.shape
    owner, read = block_owner.reshape(1, blocks), read_block.reshape(1, blocks)
    held_rows = exchange(occurrence.transpose(1, 0, 2))
    held_rows = held_rows.reshape(devices * blocks, kmers)
    own_row = jnp.concatenate(
        [slot_order, owner, jnp.zeros((1, devices - blocks), jnp.int32)], axis=1
    )
    shared = exchange(jnp.broadcast_to(own_row[:, None], (devices, 1, 2 * devices)))
    me = lax.axis_index("dev").astype(jnp.int32).reshape(1)
    listed, plan, branch = lists(me, read, shared.reshape(devices, 2 * devices))

    def finish(room):
        outgoing = pick_rows(listed, held_rows, room)
        return margins(plan, occurrence, exchange(outgoing))

    rooms = ROOMS + ((CAP - 1) * blocks,)
    return lax.switch(branch[0], [lambda room=room: finish(room) for room in rooms])


def solution(mesh):
    placed = (P("dev", None, None), P("dev", None), P("dev"), P("dev", None))

    return jax.shard_map(
        shards, mesh=mesh, in_specs=placed, out_specs=P("dev", None), check_vma=False
    )
```

```python
import jax
import jax.numpy as jnp
from jax import lax
from jax.experimental import pallas as pl
from jax.experimental.pallas import tpu as pltpu
from jax.sharding import PartitionSpec as P

CAP = 4
RB_DEV = 16
ROOMS = (128, 144)
CHUNK = 16
NOTES = 8


def spread_kernel(order_ref, owner_ref, own_ref, out_ref, wide_ref, note_ref):
    f32 = jnp.float32
    blocks, rows, lanes = own_ref.shape
    group = out_ref.shape[0]
    apart = rows + 1
    step = pl.program_id(0)

    def iota(shape, axis):
        return lax.broadcasted_iota(jnp.int32, shape, axis).astype(f32)

    @pl.when(step == 0)
    def _():
        def widen(b, carry):
            wide_ref[pl.ds(b * apart, rows), :] = own_ref[b].astype(f32)
            return carry

        lax.fori_loop(0, blocks, widen, 0, unroll=4)
        row, lane = iota((rows, lanes), 0), iota((rows, lanes), 1)
        order = order_ref[...].astype(f32)
        by_row = jnp.sum(jnp.where(row == lane, order, 0.0), axis=1, keepdims=True)
        place = jnp.sum(jnp.where(by_row == lane, row, 0.0), axis=0, keepdims=True)
        column = iota((blocks, blocks), 1)
        number = iota((blocks, blocks), 0)
        owner = owner_ref[...].astype(f32)
        owner = jnp.sum(jnp.where(number == column, owner, 0.0), axis=1, keepdims=True)
        number = iota((blocks, lanes), 0)
        held = jnp.where(owner == iota((blocks, lanes), 1), number + 1.0, 0.0)
        held = jnp.sum(held, axis=0, keepdims=True)
        rest = jnp.zeros((NOTES - 3, lanes), f32)
        note_ref[...] = jnp.concatenate([order, place, held, rest], axis=0)

    note = note_ref[...].astype(out_ref.dtype)
    for i in range(group):
        out_ref[i, :blocks] = wide_ref[pl.ds(step * group + i, blocks, stride=apart), :].astype(
            out_ref.dtype
        )
        out_ref[i, blocks:] = note


def spread(order, owner, own):
    blocks, rows, lanes = own.shape
    whole = pl.BlockSpec(memory_space=pltpu.VMEM)
    group = 16
    return pl.pallas_call(
        spread_kernel,
        grid=(rows // group,),
        in_specs=[whole, whole, whole],
        out_specs=pl.BlockSpec((group, blocks + NOTES, lanes), lambda i: (i, 0, 0)),
        out_shape=jax.ShapeDtypeStruct((rows, blocks + NOTES, lanes), own.dtype),
        scratch_shapes=[
            pltpu.VMEM((blocks * (rows + 1), lanes), jnp.float32),
            pltpu.VMEM((NOTES, lanes), jnp.float32),
        ],
        name="spread",
    )(order, owner, own)


def lists_kernel(me_ref, read_ref, note_ref, list_ref, plan_ref, most_ref, wide_ref, rank_ref, value_ref):
    f32, bf16 = jnp.float32, jnp.bfloat16
    devices = note_ref.shape[0]
    blocks = read_ref.shape[1]
    square = (devices, devices)
    most = (CAP - 1) * blocks

    def iota(shape, axis):
        return lax.broadcasted_iota(jnp.int32, shape, axis).astype(f32)

    wide_ref[...] = note_ref[...].astype(f32).reshape(devices * NOTES, devices)
    row, lane = iota(square, 0), iota(square, 1)

    def noted(n):
        return wide_ref[pl.ds(n, devices, stride=NOTES), :]

    order, place = noted(0).astype(jnp.int32), noted(1).astype(jnp.int32)
    held = noted(2).T
    there = jnp.take_along_axis(held, order, axis=1)
    number = jnp.where(there > 0.0, order.astype(f32) * (blocks + NOTES) + there, 0.0)
    values = [
        jnp.where(held > 0.0, jnp.take_along_axis(number, place ^ j, axis=1), 0.0)
        for j in range(1, CAP)
    ]
    needs = [(v > 0.0).astype(f32) for v in values]
    total = needs[0] + needs[1] + needs[2]
    below = (lane < row).astype(f32).astype(bf16)
    rank = jnp.dot(below, total.astype(bf16), preferred_element_type=f32)
    ranks = []
    for j in range(CAP - 1):
        ranks.append(jnp.where(needs[j] > 0.0, rank, -1.0))
        rank = rank + needs[j]
        rank_ref[j] = ranks[j]
        value_ref[j] = values[j] - 1.0
    count = jnp.max(rank[devices - 1 :, :])
    most_ref[0] = sum((count > room).astype(jnp.int32) for room in ROOMS)
    turn = iota((most, devices), 0)

    def fill(o, found):
        for j in range(CAP - 1):
            hit = rank_ref[j, pl.ds(o, 1), :] == turn
            found = jnp.where(hit, value_ref[j, pl.ds(o, 1), :], found)
        return found

    found = lax.fori_loop(0, devices, fill, jnp.zeros((most, devices), f32))
    list_ref[:, 0, :] = found.astype(jnp.int32)

    me = me_ref[0].astype(f32)

    def mine(array):
        return jnp.sum(jnp.where(lane == me, array, 0.0), axis=1, keepdims=True)

    reads = read_ref[...].astype(f32)
    row, column = iota((blocks, blocks), 0), iota((blocks, blocks), 1)
    read = jnp.sum(jnp.where(row == column, reads, 0.0), axis=1, keepdims=True)
    before = (read < reads) | ((read == reads) & (row < column))
    at = jnp.sum(before.astype(f32), axis=0, keepdims=True)
    own = mine(held)
    chosen = own == iota((devices, blocks), 1) + 1.0
    at = jnp.sum(jnp.where(chosen, at, 0.0), axis=1, keepdims=True)
    read = jnp.sum(jnp.where(chosen, reads, 0.0), axis=1, keepdims=True)
    turn = (at == lane) & (own > 0.0)
    stands = mine((place & (CAP - 1)).astype(f32))
    spots = [-1.0 - own] + [mine(r) for r in ranks]
    rows = []
    for j in range(CAP):
        spot = jnp.zeros_like(own)
        for p in range(CAP):
            spot = jnp.where(stands == float(p), spots[p ^ j], spot)
        rows.append(jnp.sum(jnp.where(turn, spot, 0.0), axis=0, keepdims=True))
    rows.append(jnp.sum(jnp.where(turn, own - 1.0, 0.0), axis=0, keepdims=True))
    by_read = jnp.sum(jnp.where(turn, read, 0.0), axis=0, keepdims=True)
    rows.append(jnp.where(iota((1, devices), 1) < blocks, by_read, float(RB_DEV)))
    rows += [jnp.zeros((1, devices), f32)] * 2
    plan_ref[...] = jnp.concatenate(rows, axis=0).astype(jnp.int32)


def lists(me, read, held_rows):
    devices = held_rows.shape[0]
    blocks = read.shape[1]
    small = pl.BlockSpec(memory_space=pltpu.SMEM)
    square = pltpu.VMEM((CAP - 1, devices, devices), jnp.float32)
    return pl.pallas_call(
        lists_kernel,
        grid=(1,),
        in_specs=[
            small,
            pl.BlockSpec(memory_space=pltpu.VMEM),
            pl.BlockSpec((devices, NOTES, devices), lambda i: (0, blocks // NOTES, 0)),
        ],
        out_specs=(
            pl.BlockSpec(memory_space=pltpu.VMEM),
            pl.BlockSpec(memory_space=pltpu.VMEM),
            small,
        ),
        out_shape=(
            jax.ShapeDtypeStruct(((CAP - 1) * blocks, 1, devices), jnp.int32),
            jax.ShapeDtypeStruct((8, devices), jnp.int32),
            jax.ShapeDtypeStruct((1,), jnp.int32),
        ),
        scratch_shapes=[pltpu.VMEM((devices * NOTES, devices), jnp.float32), square, square],
        name="lists",
    )(me, read, held_rows)


def pick_kernel(list_ref, rows_ref, out_ref, wide_ref, stage_ref, spare_ref, list_sem, *asked):
    group, room, lanes = out_ref.shape
    pairs = stage_ref.shape[0]

    @pl.when(pl.program_id(0) == 0)
    def _():
        copies = [
            pltpu.make_async_copy(list_ref.at[t], asked[t], list_sem) for t in range(room)
        ]
        for copy in copies:
            copy.start()
        wide_ref[...] = rows_ref[...].astype(jnp.float32)
        pltpu.make_async_copy(list_ref.at[pl.ds(0, room)], spare_ref, list_sem).wait()

    first = pl.program_id(0) * group

    def pick(i, carry):
        for u in range(pairs):
            at = i * pairs + u
            s = first + at
            for t in range(room):
                stage_ref[u, pl.ds(t, 1), :] = wide_ref[pl.ds(asked[t][0, s], 1), :]
            out_ref[at] = stage_ref[u].astype(out_ref.dtype)
        return carry

    lax.fori_loop(0, group // pairs, pick, 0)


def pick_rows(listed, rows, room):
    total, lanes = rows.shape
    devices, group, pairs = listed.shape[2], 8, 2
    return pl.pallas_call(
        pick_kernel,
        grid=(devices // group,),
        in_specs=[
            pl.BlockSpec(memory_space=pltpu.VMEM),
            pl.BlockSpec(memory_space=pltpu.VMEM),
        ],
        out_specs=pl.BlockSpec((group, room, lanes), lambda i: (i, 0, 0)),
        out_shape=jax.ShapeDtypeStruct((devices, room, lanes), rows.dtype),
        scratch_shapes=[
            pltpu.VMEM((total, lanes), jnp.float32),
            pltpu.VMEM((pairs, room, lanes), jnp.float32),
            pltpu.SMEM((room, 1, devices), jnp.int32),
            pltpu.SemaphoreType.DMA,
        ]
        + [pltpu.SMEM((1, devices), jnp.int32)] * room,
        name="pick_rows",
    )(listed, rows)


def margin_kernel(plan_ref, own_ref, got_ref, out_ref, in_ref, wide_ref, block_ref, sum_ref, other_ref, in_sem, out_sem):
    rows, room, lanes = got_ref.shape
    blocks = own_ref.shape[0]
    f32, bf16 = jnp.float32, jnp.bfloat16
    chunks = room // CHUNK
    apart = CHUNK + 1

    def fetch(c):
        return pltpu.make_async_copy(
            got_ref.at[:, pl.ds(pl.multiple_of(c * CHUNK, CHUNK), CHUNK), :], in_ref.at[c], in_sem.at[c]
        )

    for c in range(chunks):
        fetch(c).start()
    sum_ref[...] = jnp.zeros(sum_ref.shape, f32)
    other_ref[...] = jnp.zeros(other_ref.shape, f32)
    block_ref[room] = jnp.zeros((rows, lanes), bf16)

    def keep(b, carry):
        block_ref[room + 1 + b] = own_ref[b]
        return carry

    lax.fori_loop(0, blocks, keep, 0, unroll=8)

    def turn(c, carry):
        fetch(c).wait()

        def widen(d, carry):
            wide_ref[pl.ds(d * apart, CHUNK), :] = in_ref[c, d].astype(f32)
            return carry

        lax.fori_loop(0, rows, widen, 0, unroll=16)
        for t in range(CHUNK):
            block_ref[c * CHUNK + t] = wide_ref[pl.ds(t, rows, stride=apart), :].astype(bf16)
        return carry

    lax.fori_loop(0, chunks, turn, 0)

    def tiles(i):
        own = own_ref[plan_ref[CAP, i]]
        for j in range(CAP):
            spot = plan_ref[j, i]
            spot = jnp.where(spot < 0, room - 1 - spot, spot)
            yield lax.dot_general(
                own, block_ref[spot], (((1,), (1,)), ((), ())), preferred_element_type=f32
            ).astype(bf16).astype(f32)

    sums = (sum_ref, other_ref)
    unroll = 8

    def leave(r, carry):
        part = pl.ds(pl.multiple_of(r * rows, rows), rows)
        sum_ref[part] += other_ref[part]
        pltpu.make_async_copy(sum_ref.at[part], out_ref.at[part], out_sem).start()
        return carry

    def step(q, carry):
        for u in range(unroll):
            i = q * unroll + u
            part = pl.ds(pl.multiple_of(plan_ref[CAP + 1, i] * rows, rows), rows)
            for j, tile in enumerate(tiles(i)):
                sums[u % 2][part, j * rows : (j + 1) * rows] += tile
        start = jnp.where(q == 0, 0, plan_ref[CAP + 1, q * unroll])
        lax.fori_loop(start, plan_ref[CAP + 1, (q + 1) * unroll], leave, 0)
        return carry

    lax.fori_loop(0, blocks // unroll, step, 0)
    pltpu.make_async_copy(sum_ref, out_ref, out_sem).wait()


def margins(plan, own, got):
    rows, room, lanes = got.shape
    blocks = own.shape[0]
    return pl.pallas_call(
        margin_kernel,
        in_specs=[
            pl.BlockSpec(memory_space=pltpu.SMEM),
            pl.BlockSpec(memory_space=pltpu.VMEM),
            pl.BlockSpec(memory_space=pl.ANY),
        ],
        out_specs=pl.BlockSpec(memory_space=pl.ANY),
        out_shape=jax.ShapeDtypeStruct((RB_DEV * rows, CAP * rows), jnp.float32),
        scratch_shapes=[
            pltpu.VMEM((room // CHUNK, rows, CHUNK, lanes), got.dtype),
            pltpu.VMEM((rows * (CHUNK + 1), lanes), jnp.float32),
            pltpu.VMEM((room + 1 + blocks, rows, lanes), own.dtype),
            pltpu.VMEM((RB_DEV * rows, CAP * rows), jnp.float32),
            pltpu.VMEM((RB_DEV * rows, CAP * rows), jnp.float32),
            pltpu.SemaphoreType.DMA((room // CHUNK,)),
            pltpu.SemaphoreType.DMA,
        ],
        name="margins",
    )(plan, own, got)


def exchange(array):
    return lax.all_to_all(array, "dev", split_axis=0, concat_axis=0, tiled=True)


def shards(occurrence, block_owner, read_block, slot_order):
    devices = lax.axis_size("dev")
    blocks, rows, kmers = occurrence.shape
    owner, read = block_owner.reshape(1, blocks), read_block.reshape(1, blocks)
    me = lax.axis_index("dev").astype(jnp.int32).reshape(1)
    held_rows = exchange(spread(slot_order, owner, occurrence))
    listed, plan, branch = lists(me, read, held_rows)
    held_rows = held_rows.reshape(devices * (blocks + NOTES), kmers)

    def finish(room):
        outgoing = pick_rows(listed, held_rows, room)
        return margins(plan, occurrence, exchange(outgoing))

    rooms = ROOMS + ((CAP - 1) * blocks,)
    return lax.switch(branch[0], [lambda room=room: finish(room) for room in rooms])


def solution(mesh):
    placed = (P("dev", None, None), P("dev", None), P("dev"), P("dev", None))
    return jax.shard_map(
        shards, mesh=mesh, in_specs=placed, out_specs=P("dev", None), check_vma=False
    )
```

```python
import jax
import jax.numpy as jnp
from jax import lax
from jax.experimental import pallas as pl
from jax.experimental.pallas import tpu as pltpu
from jax.sharding import PartitionSpec as P

CAP = 4
RB_DEV = 16
ROOMS = (128, 144)
CHUNK = 16
NOTES = 8


def spread_kernel(order_ref, owner_ref, own_ref, out_ref, in_ref, wide_ref, note_ref, in_sem):
    f32 = jnp.float32
    blocks, rows, lanes = own_ref.shape
    group = out_ref.shape[0]
    apart = rows + 1
    step = pl.program_id(0)

    def iota(shape, axis):
        return lax.broadcasted_iota(jnp.int32, shape, axis).astype(f32)

    @pl.when(step == 0)
    def _():
        parts = [pl.ds(first, blocks // 4) for first in range(0, blocks, blocks // 4)]
        copies = [
            pltpu.make_async_copy(own_ref.at[part], in_ref.at[part], in_sem.at[c])
            for c, part in enumerate(parts)
        ]
        for copy in copies:
            copy.start()

        def widen(b, carry):
            wide_ref[pl.ds(b * apart, rows), :] = in_ref[b].astype(f32)
            return carry

        for c, copy in enumerate(copies):
            copy.wait()
            lax.fori_loop(c * (blocks // 4), (c + 1) * (blocks // 4), widen, 0, unroll=4)
        row, lane = iota((rows, lanes), 0), iota((rows, lanes), 1)
        order = order_ref[...].astype(f32)
        by_row = jnp.sum(jnp.where(row == lane, order, 0.0), axis=1, keepdims=True)
        place = jnp.sum(jnp.where(by_row == lane, row, 0.0), axis=0, keepdims=True)
        column = iota((blocks, blocks), 1)
        number = iota((blocks, blocks), 0)
        owner = owner_ref[...].astype(f32)
        owner = jnp.sum(jnp.where(number == column, owner, 0.0), axis=1, keepdims=True)
        number = iota((blocks, lanes), 0)
        held = jnp.where(owner == iota((blocks, lanes), 1), number + 1.0, 0.0)
        held = jnp.sum(held, axis=0, keepdims=True)
        rest = jnp.zeros((NOTES - 3, lanes), f32)
        note_ref[...] = jnp.concatenate([order, place, held, rest], axis=0)

    note = note_ref[...].astype(out_ref.dtype)
    for i in range(group):
        out_ref[i, :blocks] = wide_ref[pl.ds(step * group + i, blocks, stride=apart), :].astype(
            out_ref.dtype
        )
        out_ref[i, blocks:] = note


def spread(order, owner, own):
    blocks, rows, lanes = own.shape
    whole = pl.BlockSpec(memory_space=pltpu.VMEM)
    group = 32
    return pl.pallas_call(
        spread_kernel,
        grid=(rows // group,),
        in_specs=[whole, whole, pl.BlockSpec(memory_space=pl.ANY)],
        out_specs=pl.BlockSpec((group, blocks + NOTES, lanes), lambda i: (i, 0, 0)),
        out_shape=jax.ShapeDtypeStruct((rows, blocks + NOTES, lanes), own.dtype),
        scratch_shapes=[
            pltpu.VMEM(own.shape, own.dtype),
            pltpu.VMEM((blocks * (rows + 1), lanes), jnp.float32),
            pltpu.VMEM((NOTES, lanes), jnp.float32),
            pltpu.SemaphoreType.DMA((4,)),
        ],
        name="spread",
    )(order, owner, own)


def lists_kernel(note_ref, list_ref, most_ref, held_ref, place_ref, rank_ref, wide_ref, value_ref):
    f32, bf16 = jnp.float32, jnp.bfloat16
    devices = note_ref.shape[0]
    square = (devices, devices)
    most = list_ref.shape[0]
    blocks = most // (CAP - 1)

    def iota(shape, axis):
        return lax.broadcasted_iota(jnp.int32, shape, axis).astype(f32)

    wide_ref[...] = note_ref[...].astype(f32).reshape(devices * NOTES, devices)
    row, lane = iota(square, 0), iota(square, 1)

    def noted(n):
        return wide_ref[pl.ds(n, devices, stride=NOTES), :]

    order, place = noted(0).astype(jnp.int32), noted(1).astype(jnp.int32)
    held = noted(2).T
    held_ref[...] = held
    place_ref[...] = place
    there = jnp.take_along_axis(held, order, axis=1)
    number = jnp.where(there > 0.0, order.astype(f32) * (blocks + NOTES) + there, 0.0)
    values = [
        jnp.where(held > 0.0, jnp.take_along_axis(number, place ^ j, axis=1), 0.0)
        for j in range(1, CAP)
    ]
    needs = [(v > 0.0).astype(f32) for v in values]
    total = needs[0] + needs[1] + needs[2]
    below = (lane < row).astype(f32).astype(bf16)
    rank = jnp.dot(below, total.astype(bf16), preferred_element_type=f32)
    for j in range(CAP - 1):
        rank_ref[j] = jnp.where(needs[j] > 0.0, rank, -1.0)
        rank = rank + needs[j]
        value_ref[j] = values[j] - 1.0
    count = jnp.max(rank[devices - 1 :, :])
    most_ref[0] = sum((count > room).astype(jnp.int32) for room in ROOMS)

    def entries(first, length):
        turn = iota((length, devices), 0) + float(first)

        def fill(o, found):
            for j in range(CAP - 1):
                hit = rank_ref[j, pl.ds(o, 1), :] == turn
                found = jnp.where(hit, value_ref[j, pl.ds(o, 1), :], found)
            return found

        found = lax.fori_loop(0, devices, fill, jnp.zeros((length, devices), f32), unroll=2)
        list_ref[first : first + length, 0, :] = found.astype(jnp.int32)

    entries(0, devices)

    @pl.when(count > devices)
    def _():
        entries(devices, most - devices)


def plan_kernel(me_ref, read_ref, held_ref, place_ref, rank_ref, plan_ref):
    f32 = jnp.float32
    devices = held_ref.shape[0]
    blocks = read_ref.shape[1]

    def iota(shape, axis):
        return lax.broadcasted_iota(jnp.int32, shape, axis).astype(f32)

    lane = iota((devices, devices), 1)
    me = me_ref[0].astype(f32)

    def mine(array):
        return jnp.sum(jnp.where(lane == me, array, 0.0), axis=1, keepdims=True)

    reads = read_ref[...].astype(f32)
    row, column = iota((blocks, blocks), 0), iota((blocks, blocks), 1)
    read = jnp.sum(jnp.where(row == column, reads, 0.0), axis=1, keepdims=True)
    before = (read < reads) | ((read == reads) & (row < column))
    at = jnp.sum(before.astype(f32), axis=0, keepdims=True)
    own = mine(held_ref[...])
    chosen = own == iota((devices, blocks), 1) + 1.0
    at = jnp.sum(jnp.where(chosen, at, 0.0), axis=1, keepdims=True)
    read = jnp.sum(jnp.where(chosen, reads, 0.0), axis=1, keepdims=True)
    turn = (at == lane) & (own > 0.0)
    stands = mine((place_ref[...] & (CAP - 1)).astype(f32))
    spots = [-1.0 - own] + [mine(rank_ref[j]) for j in range(CAP - 1)]
    rows = []
    for j in range(CAP):
        spot = jnp.zeros_like(own)
        for p in range(CAP):
            spot = jnp.where(stands == float(p), spots[p ^ j], spot)
        rows.append(jnp.sum(jnp.where(turn, spot, 0.0), axis=0, keepdims=True))
    rows.append(jnp.sum(jnp.where(turn, own - 1.0, 0.0), axis=0, keepdims=True))
    by_read = jnp.sum(jnp.where(turn, read, 0.0), axis=0, keepdims=True)
    rows.append(jnp.where(iota((1, devices), 1) < blocks, by_read, float(RB_DEV)))
    rows += [jnp.zeros((1, devices), f32)] * 2
    plan_ref[...] = jnp.concatenate(rows, axis=0).astype(jnp.int32)


def lists(held_rows, blocks):
    devices = held_rows.shape[0]
    whole = pl.BlockSpec(memory_space=pltpu.VMEM)
    small = pl.BlockSpec(memory_space=pltpu.SMEM)
    square = (devices, devices)
    return pl.pallas_call(
        lists_kernel,
        grid=(1,),
        in_specs=[pl.BlockSpec((devices, NOTES, devices), lambda i: (0, blocks // NOTES, 0))],
        out_specs=(whole, small, whole, whole, whole),
        out_shape=(
            jax.ShapeDtypeStruct(((CAP - 1) * blocks, 1, devices), jnp.int32),
            jax.ShapeDtypeStruct((1,), jnp.int32),
            jax.ShapeDtypeStruct(square, jnp.float32),
            jax.ShapeDtypeStruct(square, jnp.int32),
            jax.ShapeDtypeStruct((CAP - 1,) + square, jnp.float32),
        ),
        scratch_shapes=[
            pltpu.VMEM((devices * NOTES, devices), jnp.float32),
            pltpu.VMEM((CAP - 1,) + square, jnp.float32),
        ],
        name="lists",
    )(held_rows)


def planned(me, read, held, place, ranks):
    whole = pl.BlockSpec(memory_space=pltpu.VMEM)
    return pl.pallas_call(
        plan_kernel,
        in_specs=[pl.BlockSpec(memory_space=pltpu.SMEM)] + [whole] * 4,
        out_specs=whole,
        out_shape=jax.ShapeDtypeStruct((8, held.shape[0]), jnp.int32),
        name="plan",
    )(me, read, held, place, ranks)


def pick_kernel(list_ref, rows_ref, out_ref, wide_ref, stage_ref, spare_ref, list_sem, *asked):
    group, room, lanes = out_ref.shape
    pairs = stage_ref.shape[0]

    @pl.when(pl.program_id(0) == 0)
    def _():
        copies = [
            pltpu.make_async_copy(list_ref.at[t], asked[t], list_sem) for t in range(room)
        ]
        for copy in copies:
            copy.start()
        wide_ref[...] = rows_ref[...].astype(jnp.float32)
        pltpu.make_async_copy(list_ref.at[pl.ds(0, room)], spare_ref, list_sem).wait()

    first = pl.program_id(0) * group

    def pick(i, carry):
        for u in range(pairs):
            at = i * pairs + u
            s = first + at
            for t in range(room):
                stage_ref[u, pl.ds(t, 1), :] = wide_ref[pl.ds(asked[t][0, s], 1), :]
            out_ref[at] = stage_ref[u].astype(out_ref.dtype)
        return carry

    lax.fori_loop(0, group // pairs, pick, 0)


def pick_rows(listed, rows, room):
    total, lanes = rows.shape
    devices, group, pairs = listed.shape[2], 16, 2
    return pl.pallas_call(
        pick_kernel,
        grid=(devices // group,),
        in_specs=[
            pl.BlockSpec(memory_space=pltpu.VMEM),
            pl.BlockSpec(memory_space=pltpu.VMEM),
        ],
        out_specs=pl.BlockSpec((group, room, lanes), lambda i: (i, 0, 0)),
        out_shape=jax.ShapeDtypeStruct((devices, room, lanes), rows.dtype),
        scratch_shapes=[
            pltpu.VMEM((total, lanes), jnp.float32),
            pltpu.VMEM((pairs, room, lanes), jnp.float32),
            pltpu.SMEM((room, 1, devices), jnp.int32),
            pltpu.SemaphoreType.DMA,
        ]
        + [pltpu.SMEM((1, devices), jnp.int32)] * room,
        name="pick_rows",
    )(listed, rows)


def margin_kernel(plan_ref, own_ref, got_ref, out_ref, in_ref, wide_ref, block_ref, sum_ref, other_ref, in_sem, out_sem):
    rows, room, lanes = got_ref.shape
    blocks = own_ref.shape[0]
    f32, bf16 = jnp.float32, jnp.bfloat16
    chunks = room // CHUNK
    apart = CHUNK + 1

    def fetch(c):
        return pltpu.make_async_copy(
            got_ref.at[:, pl.ds(pl.multiple_of(c * CHUNK, CHUNK), CHUNK), :], in_ref.at[c], in_sem.at[c]
        )

    for c in range(chunks):
        fetch(c).start()
    sum_ref[...] = jnp.zeros(sum_ref.shape, f32)
    other_ref[...] = jnp.zeros(other_ref.shape, f32)
    block_ref[room] = jnp.zeros((rows, lanes), bf16)

    def keep(b, carry):
        block_ref[room + 1 + b] = own_ref[b]
        return carry

    lax.fori_loop(0, blocks, keep, 0, unroll=8)

    def turn(c, carry):
        fetch(c).wait()

        def widen(d, carry):
            wide_ref[pl.ds(d * apart, CHUNK), :] = in_ref[c, d].astype(f32)
            return carry

        lax.fori_loop(0, rows, widen, 0, unroll=16)
        for t in range(CHUNK):
            block_ref[c * CHUNK + t] = wide_ref[pl.ds(t, rows, stride=apart), :].astype(bf16)
        return carry

    lax.fori_loop(0, chunks, turn, 0)

    def tiles(i):
        own = own_ref[plan_ref[CAP, i]]
        for j in range(CAP):
            spot = plan_ref[j, i]
            spot = jnp.where(spot < 0, room - 1 - spot, spot)
            yield lax.dot_general(
                own, block_ref[spot], (((1,), (1,)), ((), ())), preferred_element_type=f32
            ).astype(bf16).astype(f32)

    sums = (sum_ref, other_ref)
    unroll = 8

    def leave(r, carry):
        part = pl.ds(pl.multiple_of(r * rows, rows), rows)
        sum_ref[part] += other_ref[part]
        pltpu.make_async_copy(sum_ref.at[part], out_ref.at[part], out_sem).start()
        return carry

    def step(q, carry):
        for u in range(unroll):
            i = q * unroll + u
            part = pl.ds(pl.multiple_of(plan_ref[CAP + 1, i] * rows, rows), rows)
            for j, tile in enumerate(tiles(i)):
                sums[u % 2][part, j * rows : (j + 1) * rows] += tile
        start = jnp.where(q == 0, 0, plan_ref[CAP + 1, q * unroll])
        lax.fori_loop(start, plan_ref[CAP + 1, (q + 1) * unroll], leave, 0)
        return carry

    lax.fori_loop(0, blocks // unroll, step, 0)
    pltpu.make_async_copy(sum_ref, out_ref, out_sem).wait()


def margins(plan, own, got):
    rows, room, lanes = got.shape
    blocks = own.shape[0]
    return pl.pallas_call(
        margin_kernel,
        in_specs=[
            pl.BlockSpec(memory_space=pltpu.SMEM),
            pl.BlockSpec(memory_space=pltpu.VMEM),
            pl.BlockSpec(memory_space=pl.ANY),
        ],
        out_specs=pl.BlockSpec(memory_space=pl.ANY),
        out_shape=jax.ShapeDtypeStruct((RB_DEV * rows, CAP * rows), jnp.float32),
        scratch_shapes=[
            pltpu.VMEM((room // CHUNK, rows, CHUNK, lanes), got.dtype),
            pltpu.VMEM((rows * (CHUNK + 1), lanes), jnp.float32),
            pltpu.VMEM((room + 1 + blocks, rows, lanes), own.dtype),
            pltpu.VMEM((RB_DEV * rows, CAP * rows), jnp.float32),
            pltpu.VMEM((RB_DEV * rows, CAP * rows), jnp.float32),
            pltpu.SemaphoreType.DMA((room // CHUNK,)),
            pltpu.SemaphoreType.DMA,
        ],
        name="margins",
    )(plan, own, got)


def exchange(array):
    return lax.all_to_all(array, "dev", split_axis=0, concat_axis=0, tiled=True)


def shards(occurrence, block_owner, read_block, slot_order):
    devices = lax.axis_size("dev")
    blocks, rows, kmers = occurrence.shape
    owner, read = block_owner.reshape(1, blocks), read_block.reshape(1, blocks)
    me = lax.axis_index("dev").astype(jnp.int32).reshape(1)
    held_rows = exchange(spread(slot_order, owner, occurrence))
    listed, branch, held, place, ranks = lists(held_rows, blocks)
    held_rows = held_rows.reshape(devices * (blocks + NOTES), kmers)

    def finish(room):
        outgoing = pick_rows(listed, held_rows, room)
        plan = planned(me, read, held, place, ranks)
        return margins(plan, occurrence, exchange(outgoing))

    rooms = ROOMS + ((CAP - 1) * blocks,)
    return lax.switch(branch[0], [lambda room=room: finish(room) for room in rooms])


def solution(mesh):
    placed = (P("dev", None, None), P("dev", None), P("dev"), P("dev", None))
    return jax.shard_map(
        shards, mesh=mesh, in_specs=placed, out_specs=P("dev", None), check_vma=False
    )
```

```python
import jax
import jax.numpy as jnp
from jax import lax
from jax.experimental import pallas as pl
from jax.experimental.pallas import tpu as pltpu
from jax.sharding import PartitionSpec as P

CAP = 4
RB_DEV = 16
ROOMS = (128, 144)
CHUNK = 16
NOTES = 8


def spread_kernel(order_ref, owner_ref, own_ref, out_ref, in_ref, wide_ref, note_ref, in_sem):
    f32 = jnp.float32
    blocks, rows, lanes = own_ref.shape
    group = out_ref.shape[0]
    apart = rows + 1
    step = pl.program_id(0)

    def iota(shape, axis):
        return lax.broadcasted_iota(jnp.int32, shape, axis).astype(f32)

    @pl.when(step == 0)
    def _():
        parts = [pl.ds(first, blocks // 4) for first in range(0, blocks, blocks // 4)]
        copies = [
            pltpu.make_async_copy(own_ref.at[part], in_ref.at[part], in_sem.at[c])
            for c, part in enumerate(parts)
        ]
        for copy in copies:
            copy.start()

        def widen(b, carry):
            wide_ref[pl.ds(b * apart, rows), :] = in_ref[b].astype(f32)
            return carry

        for c, copy in enumerate(copies):
            copy.wait()
            lax.fori_loop(c * (blocks // 4), (c + 1) * (blocks // 4), widen, 0, unroll=4)
        row, lane = iota((rows, lanes), 0), iota((rows, lanes), 1)
        order = order_ref[...].astype(f32)
        by_row = jnp.sum(jnp.where(row == lane, order, 0.0), axis=1, keepdims=True)
        place = jnp.sum(jnp.where(by_row == lane, row, 0.0), axis=0, keepdims=True)
        column = iota((blocks, blocks), 1)
        number = iota((blocks, blocks), 0)
        owner = owner_ref[...].astype(f32)
        owner = jnp.sum(jnp.where(number == column, owner, 0.0), axis=1, keepdims=True)
        number = iota((blocks, lanes), 0)
        held = jnp.where(owner == iota((blocks, lanes), 1), number + 1.0, 0.0)
        held = jnp.sum(held, axis=0, keepdims=True)
        rest = jnp.zeros((NOTES - 3, lanes), f32)
        note_ref[...] = jnp.concatenate([order, place, held, rest], axis=0)

    note = note_ref[...].astype(out_ref.dtype)
    for i in range(group):
        out_ref[i, :blocks] = wide_ref[pl.ds(step * group + i, blocks, stride=apart), :].astype(
            out_ref.dtype
        )
        out_ref[i, blocks:] = note


def spread(order, owner, own):
    blocks, rows, lanes = own.shape
    whole = pl.BlockSpec(memory_space=pltpu.VMEM)
    group = 32
    return pl.pallas_call(
        spread_kernel,
        grid=(rows // group,),
        in_specs=[whole, whole, pl.BlockSpec(memory_space=pl.ANY)],
        out_specs=pl.BlockSpec((group, blocks + NOTES, lanes), lambda i: (i, 0, 0)),
        out_shape=jax.ShapeDtypeStruct((rows, blocks + NOTES, lanes), own.dtype),
        scratch_shapes=[
            pltpu.VMEM(own.shape, own.dtype),
            pltpu.VMEM((blocks * (rows + 1), lanes), jnp.float32),
            pltpu.VMEM((NOTES, lanes), jnp.float32),
            pltpu.SemaphoreType.DMA((4,)),
        ],
        name="spread",
    )(order, owner, own)


def lists_kernel(note_ref, list_ref, most_ref, held_ref, place_ref, rank_ref, wide_ref, value_ref):
    f32, bf16 = jnp.float32, jnp.bfloat16
    devices = note_ref.shape[0]
    square = (devices, devices)
    most = list_ref.shape[0]
    blocks = most // (CAP - 1)

    def iota(shape, axis):
        return lax.broadcasted_iota(jnp.int32, shape, axis).astype(f32)

    wide_ref[...] = note_ref[...].astype(f32).reshape(devices * NOTES, devices)
    row, lane = iota(square, 0), iota(square, 1)

    def noted(n):
        return wide_ref[pl.ds(n, devices, stride=NOTES), :]

    order, place = noted(0).astype(jnp.int32), noted(1).astype(jnp.int32)
    held = noted(2).T
    held_ref[...] = held
    place_ref[...] = place
    there = jnp.take_along_axis(held, order, axis=1)
    number = jnp.where(there > 0.0, order.astype(f32) * (blocks + NOTES) + there, 0.0)
    values = [
        jnp.where(held > 0.0, jnp.take_along_axis(number, place ^ j, axis=1), 0.0)
        for j in range(1, CAP)
    ]
    needs = [(v > 0.0).astype(f32) for v in values]
    total = needs[0] + needs[1] + needs[2]
    below = (lane < row).astype(f32).astype(bf16)
    rank = jnp.dot(below, total.astype(bf16), preferred_element_type=f32)
    for j in range(CAP - 1):
        rank_ref[j] = jnp.where(needs[j] > 0.0, rank, -1.0)
        rank = rank + needs[j]
        value_ref[j] = values[j] - 1.0
    count = jnp.max(rank[devices - 1 :, :])
    most_ref[0] = sum((count > room).astype(jnp.int32) for room in ROOMS)

    def entries(first, length):
        turn = iota((length, devices), 0) + float(first)

        def fill(o, found):
            for j in range(CAP - 1):
                hit = rank_ref[j, pl.ds(o, 1), :] == turn
                found = jnp.where(hit, value_ref[j, pl.ds(o, 1), :], found)
            return found

        found = lax.fori_loop(0, devices, fill, jnp.zeros((length, devices), f32), unroll=2)
        list_ref[first : first + length, 0, :] = found.astype(jnp.int32)

    entries(0, devices)

    @pl.when(count > devices)
    def _():
        entries(devices, most - devices)


def plan_kernel(me_ref, read_ref, held_ref, place_ref, rank_ref, plan_ref):
    f32 = jnp.float32
    devices = held_ref.shape[0]
    blocks = read_ref.shape[1]

    def iota(shape, axis):
        return lax.broadcasted_iota(jnp.int32, shape, axis).astype(f32)

    lane = iota((devices, devices), 1)
    me = me_ref[0].astype(f32)

    def mine(array):
        return jnp.sum(jnp.where(lane == me, array, 0.0), axis=1, keepdims=True)

    reads = read_ref[...].astype(f32)
    row, column = iota((blocks, blocks), 0), iota((blocks, blocks), 1)
    read = jnp.sum(jnp.where(row == column, reads, 0.0), axis=1, keepdims=True)
    before = (read < reads) | ((read == reads) & (row < column))
    at = jnp.sum(before.astype(f32), axis=0, keepdims=True)
    own = mine(held_ref[...])
    chosen = own == iota((devices, blocks), 1) + 1.0
    at = jnp.sum(jnp.where(chosen, at, 0.0), axis=1, keepdims=True)
    read = jnp.sum(jnp.where(chosen, reads, 0.0), axis=1, keepdims=True)
    turn = (at == lane) & (own > 0.0)
    stands = mine((place_ref[...] & (CAP - 1)).astype(f32))
    spots = [-1.0 - own] + [mine(rank_ref[j]) for j in range(CAP - 1)]
    rows = []
    for j in range(CAP):
        spot = jnp.zeros_like(own)
        for p in range(CAP):
            spot = jnp.where(stands == float(p), spots[p ^ j], spot)
        rows.append(jnp.sum(jnp.where(turn, spot, 0.0), axis=0, keepdims=True))
    rows.append(jnp.sum(jnp.where(turn, own - 1.0, 0.0), axis=0, keepdims=True))
    by_read = jnp.sum(jnp.where(turn, read, 0.0), axis=0, keepdims=True)
    rows.append(jnp.where(iota((1, devices), 1) < blocks, by_read, float(RB_DEV)))
    rows += [jnp.zeros((1, devices), f32)] * 2
    plan_ref[...] = jnp.concatenate(rows, axis=0).astype(jnp.int32)


def lists(held_rows, blocks):
    devices = held_rows.shape[0]
    whole = pl.BlockSpec(memory_space=pltpu.VMEM)
    small = pl.BlockSpec(memory_space=pltpu.SMEM)
    square = (devices, devices)
    return pl.pallas_call(
        lists_kernel,
        grid=(1,),
        in_specs=[pl.BlockSpec((devices, NOTES, devices), lambda i: (0, blocks // NOTES, 0))],
        out_specs=(whole, small, whole, whole, whole),
        out_shape=(
            jax.ShapeDtypeStruct(((CAP - 1) * blocks, 1, devices), jnp.int32),
            jax.ShapeDtypeStruct((1,), jnp.int32),
            jax.ShapeDtypeStruct(square, jnp.float32),
            jax.ShapeDtypeStruct(square, jnp.int32),
            jax.ShapeDtypeStruct((CAP - 1,) + square, jnp.float32),
        ),
        scratch_shapes=[
            pltpu.VMEM((devices * NOTES, devices), jnp.float32),
            pltpu.VMEM((CAP - 1,) + square, jnp.float32),
        ],
        name="lists",
    )(held_rows)


def planned(me, read, held, place, ranks):
    whole = pl.BlockSpec(memory_space=pltpu.VMEM)
    return pl.pallas_call(
        plan_kernel,
        in_specs=[pl.BlockSpec(memory_space=pltpu.SMEM)] + [whole] * 4,
        out_specs=whole,
        out_shape=jax.ShapeDtypeStruct((8, held.shape[0]), jnp.int32),
        name="plan",
    )(me, read, held, place, ranks)


def pick_kernel(list_ref, rows_ref, out_ref, wide_ref, stage_ref, spare_ref, list_sem, *asked):
    group, room, lanes = out_ref.shape
    pairs = stage_ref.shape[0]

    @pl.when(pl.program_id(0) == 0)
    def _():
        copies = [
            pltpu.make_async_copy(list_ref.at[t], asked[t], list_sem) for t in range(room)
        ]
        for copy in copies:
            copy.start()
        wide_ref[...] = rows_ref[...].astype(jnp.float32)
        pltpu.make_async_copy(list_ref.at[pl.ds(0, room)], spare_ref, list_sem).wait()

    first = pl.program_id(0) * group

    def pick(i, carry):
        for u in range(pairs):
            at = i * pairs + u
            s = first + at
            for t in range(room):
                stage_ref[u, pl.ds(t, 1), :] = wide_ref[pl.ds(asked[t][0, s], 1), :]
            out_ref[at] = stage_ref[u].astype(out_ref.dtype)
        return carry

    lax.fori_loop(0, group // pairs, pick, 0)


def pick_rows(listed, rows, room):
    total, lanes = rows.shape
    devices, group, pairs = listed.shape[2], 16, 2
    return pl.pallas_call(
        pick_kernel,
        grid=(devices // group,),
        in_specs=[
            pl.BlockSpec(memory_space=pltpu.VMEM),
            pl.BlockSpec(memory_space=pltpu.VMEM),
        ],
        out_specs=pl.BlockSpec((group, room, lanes), lambda i: (i, 0, 0)),
        out_shape=jax.ShapeDtypeStruct((devices, room, lanes), rows.dtype),
        scratch_shapes=[
            pltpu.VMEM((total, lanes), jnp.float32),
            pltpu.VMEM((pairs, room, lanes), jnp.float32),
            pltpu.SMEM((room, 1, devices), jnp.int32),
            pltpu.SemaphoreType.DMA,
        ]
        + [pltpu.SMEM((1, devices), jnp.int32)] * room,
        name="pick_rows",
    )(listed, rows)


def margin_kernel(plan_ref, own_ref, got_ref, out_ref, in_ref, wide_ref, block_ref, sum_ref, other_ref, in_sem, out_sem):
    rows, room, lanes = got_ref.shape
    blocks = own_ref.shape[0]
    f32, bf16 = jnp.float32, jnp.bfloat16
    chunks = room // CHUNK
    apart = CHUNK + 1

    def fetch(c):
        return pltpu.make_async_copy(
            got_ref.at[:, pl.ds(pl.multiple_of(c * CHUNK, CHUNK), CHUNK), :], in_ref.at[c], in_sem.at[c]
        )

    for c in range(chunks):
        fetch(c).start()
    sum_ref[...] = jnp.zeros(sum_ref.shape, f32)
    other_ref[...] = jnp.zeros(other_ref.shape, f32)
    block_ref[room] = jnp.zeros((rows, lanes), bf16)

    def keep(b, carry):
        block_ref[room + 1 + b] = own_ref[b]
        return carry

    lax.fori_loop(0, blocks, keep, 0, unroll=8)

    def turn(c, carry):
        fetch(c).wait()

        def widen(d, carry):
            wide_ref[pl.ds(d * apart, CHUNK), :] = in_ref[c, d].astype(f32)
            return carry

        lax.fori_loop(0, rows, widen, 0, unroll=16)
        for t in range(CHUNK):
            block_ref[c * CHUNK + t] = wide_ref[pl.ds(t, rows, stride=apart), :].astype(bf16)
        return carry

    lax.fori_loop(0, chunks, turn, 0)

    def tiles(i):
        own = own_ref[plan_ref[CAP, i]]
        spots = [plan_ref[j, i] for j in range(CAP)]
        spots = [jnp.where(spot < 0, room - 1 - spot, spot) for spot in spots]
        for j in range(0, CAP, 2):
            pair = jnp.concatenate([block_ref[spots[j]], block_ref[spots[j + 1]]], axis=0)
            tile = lax.dot_general(own, pair, (((1,), (1,)), ((), ())), preferred_element_type=f32)
            yield tile.astype(bf16).astype(f32)

    sums = (sum_ref, other_ref)
    unroll = 8

    def leave(r, carry):
        part = pl.ds(pl.multiple_of(r * rows, rows), rows)
        sum_ref[part] += other_ref[part]
        pltpu.make_async_copy(sum_ref.at[part], out_ref.at[part], out_sem).start()
        return carry

    def step(q, carry):
        for u in range(unroll):
            i = q * unroll + u
            part = pl.ds(pl.multiple_of(plan_ref[CAP + 1, i] * rows, rows), rows)
            for j, tile in enumerate(tiles(i)):
                sums[u % 2][part, 2 * j * rows : 2 * (j + 1) * rows] += tile
        start = jnp.where(q == 0, 0, plan_ref[CAP + 1, q * unroll])
        lax.fori_loop(start, plan_ref[CAP + 1, (q + 1) * unroll], leave, 0)
        return carry

    lax.fori_loop(0, blocks // unroll, step, 0)
    pltpu.make_async_copy(sum_ref, out_ref, out_sem).wait()


def margins(plan, own, got):
    rows, room, lanes = got.shape
    blocks = own.shape[0]
    return pl.pallas_call(
        margin_kernel,
        in_specs=[
            pl.BlockSpec(memory_space=pltpu.SMEM),
            pl.BlockSpec(memory_space=pltpu.VMEM),
            pl.BlockSpec(memory_space=pl.ANY),
        ],
        out_specs=pl.BlockSpec(memory_space=pl.ANY),
        out_shape=jax.ShapeDtypeStruct((RB_DEV * rows, CAP * rows), jnp.float32),
        scratch_shapes=[
            pltpu.VMEM((room // CHUNK, rows, CHUNK, lanes), got.dtype),
            pltpu.VMEM((rows * (CHUNK + 1), lanes), jnp.float32),
            pltpu.VMEM((room + 1 + blocks, rows, lanes), own.dtype),
            pltpu.VMEM((RB_DEV * rows, CAP * rows), jnp.float32),
            pltpu.VMEM((RB_DEV * rows, CAP * rows), jnp.float32),
            pltpu.SemaphoreType.DMA((room // CHUNK,)),
            pltpu.SemaphoreType.DMA,
        ],
        name="margins",
    )(plan, own, got)


def exchange(array):
    return lax.all_to_all(array, "dev", split_axis=0, concat_axis=0, tiled=True)


def shards(occurrence, block_owner, read_block, slot_order):
    devices = lax.axis_size("dev")
    blocks, rows, kmers = occurrence.shape
    owner, read = block_owner.reshape(1, blocks), read_block.reshape(1, blocks)
    me = lax.axis_index("dev").astype(jnp.int32).reshape(1)
    held_rows = exchange(spread(slot_order, owner, occurrence))
    listed, branch, held, place, ranks = lists(held_rows, blocks)
    held_rows = held_rows.reshape(devices * (blocks + NOTES), kmers)

    def finish(room):
        outgoing = pick_rows(listed, held_rows, room)
        plan = planned(me, read, held, place, ranks)
        return margins(plan, occurrence, exchange(outgoing))

    rooms = ROOMS + ((CAP - 1) * blocks,)
    return lax.switch(branch[0], [lambda room=room: finish(room) for room in rooms])


def solution(mesh):
    placed = (P("dev", None, None), P("dev", None), P("dev"), P("dev", None))
    return jax.shard_map(
        shards, mesh=mesh, in_specs=placed, out_specs=P("dev", None), check_vma=False
    )
```

```python
import jax
import jax.numpy as jnp
from jax import lax
from jax.experimental import pallas as pl
from jax.experimental.pallas import tpu as pltpu
from jax.sharding import PartitionSpec as P

CAP = 4
RB_DEV = 16
ROOMS = (128, 144)
CHUNK = 16
NOTES = 8


def spread_kernel(order_ref, owner_ref, own_ref, out_ref, in_ref, wide_ref, note_ref, in_sem):
    f32 = jnp.float32
    blocks, rows, lanes = own_ref.shape
    group = out_ref.shape[0]
    apart = rows + 1
    step = pl.program_id(0)

    def iota(shape, axis):
        return lax.broadcasted_iota(jnp.int32, shape, axis).astype(f32)

    @pl.when(step == 0)
    def _():
        parts = [pl.ds(first, blocks // 4) for first in range(0, blocks, blocks // 4)]
        copies = [
            pltpu.make_async_copy(own_ref.at[part], in_ref.at[part], in_sem.at[c])
            for c, part in enumerate(parts)
        ]
        for copy in copies:
            copy.start()

        def widen(b, carry):
            wide_ref[pl.ds(b * apart, rows), :] = in_ref[b].astype(f32)
            return carry

        for c, copy in enumerate(copies):
            copy.wait()
            lax.fori_loop(c * (blocks // 4), (c + 1) * (blocks // 4), widen, 0, unroll=4)
        row, lane = iota((rows, lanes), 0), iota((rows, lanes), 1)
        order = order_ref[...].astype(f32)
        by_row = jnp.sum(jnp.where(row == lane, order, 0.0), axis=1, keepdims=True)
        place = jnp.sum(jnp.where(by_row == lane, row, 0.0), axis=0, keepdims=True)
        column = iota((blocks, blocks), 1)
        number = iota((blocks, blocks), 0)
        owner = owner_ref[...].astype(f32)
        owner = jnp.sum(jnp.where(number == column, owner, 0.0), axis=1, keepdims=True)
        number = iota((blocks, lanes), 0)
        held = jnp.where(owner == iota((blocks, lanes), 1), number + 1.0, 0.0)
        held = jnp.sum(held, axis=0, keepdims=True)
        rest = jnp.zeros((NOTES - 3, lanes), f32)
        note_ref[...] = jnp.concatenate([order, place, held, rest], axis=0)

    note = note_ref[...].astype(out_ref.dtype)
    for i in range(group):
        out_ref[i, :blocks] = wide_ref[pl.ds(step * group + i, blocks, stride=apart), :].astype(
            out_ref.dtype
        )
        out_ref[i, blocks:] = note


def spread(order, owner, own):
    blocks, rows, lanes = own.shape
    whole = pl.BlockSpec(memory_space=pltpu.VMEM)
    group = 32
    return pl.pallas_call(
        spread_kernel,
        grid=(rows // group,),
        in_specs=[whole, whole, pl.BlockSpec(memory_space=pl.ANY)],
        out_specs=pl.BlockSpec((group, blocks + NOTES, lanes), lambda i: (i, 0, 0)),
        out_shape=jax.ShapeDtypeStruct((rows, blocks + NOTES, lanes), own.dtype),
        scratch_shapes=[
            pltpu.VMEM(own.shape, own.dtype),
            pltpu.VMEM((blocks * (rows + 1), lanes), jnp.float32),
            pltpu.VMEM((NOTES, lanes), jnp.float32),
            pltpu.SemaphoreType.DMA((4,)),
        ],
        name="spread",
    )(order, owner, own)


def lists_kernel(note_ref, list_ref, most_ref, held_ref, place_ref, rank_ref, wide_ref, value_ref):
    f32, bf16 = jnp.float32, jnp.bfloat16
    devices = note_ref.shape[0]
    square = (devices, devices)
    most = list_ref.shape[0]
    blocks = most // (CAP - 1)

    def iota(shape, axis):
        return lax.broadcasted_iota(jnp.int32, shape, axis).astype(f32)

    wide_ref[...] = note_ref[...].astype(f32).reshape(devices * NOTES, devices)
    row, lane = iota(square, 0), iota(square, 1)

    def noted(n):
        return wide_ref[pl.ds(n, devices, stride=NOTES), :]

    order, place = noted(0).astype(jnp.int32), noted(1).astype(jnp.int32)
    held = noted(2).T
    held_ref[...] = held
    place_ref[...] = place
    there = jnp.take_along_axis(held, order, axis=1)
    number = jnp.where(there > 0.0, order.astype(f32) * (blocks + NOTES) + there, 0.0)
    values = [
        jnp.where(held > 0.0, jnp.take_along_axis(number, place ^ j, axis=1), 0.0)
        for j in range(1, CAP)
    ]
    needs = [(v > 0.0).astype(f32) for v in values]
    total = needs[0] + needs[1] + needs[2]
    below = (lane < row).astype(f32).astype(bf16)
    rank = jnp.dot(below, total.astype(bf16), preferred_element_type=f32)
    for j in range(CAP - 1):
        rank_ref[j] = jnp.where(needs[j] > 0.0, rank, -1.0)
        rank = rank + needs[j]
        value_ref[j] = values[j] - 1.0
    count = jnp.max(rank[devices - 1 :, :])
    most_ref[0] = sum((count > room).astype(jnp.int32) for room in ROOMS)

    def entries(first, length):
        turn = iota((length, devices), 0) + float(first)

        def fill(o, found):
            for j in range(CAP - 1):
                hit = rank_ref[j, pl.ds(o, 1), :] == turn
                found = jnp.where(hit, value_ref[j, pl.ds(o, 1), :], found)
            return found

        found = lax.fori_loop(0, devices, fill, jnp.zeros((length, devices), f32), unroll=2)
        list_ref[first : first + length, 0, :] = found.astype(jnp.int32)

    entries(0, devices)

    @pl.when(count > devices)
    def _():
        entries(devices, most - devices)


def plan_kernel(me_ref, read_ref, held_ref, place_ref, rank_ref, plan_ref):
    f32 = jnp.float32
    devices = held_ref.shape[0]
    blocks = read_ref.shape[1]

    def iota(shape, axis):
        return lax.broadcasted_iota(jnp.int32, shape, axis).astype(f32)

    lane = iota((devices, devices), 1)
    me = me_ref[0].astype(f32)

    def mine(array):
        return jnp.sum(jnp.where(lane == me, array, 0.0), axis=1, keepdims=True)

    reads = read_ref[...].astype(f32)
    row, column = iota((blocks, blocks), 0), iota((blocks, blocks), 1)
    read = jnp.sum(jnp.where(row == column, reads, 0.0), axis=1, keepdims=True)
    before = (read < reads) | ((read == reads) & (row < column))
    at = jnp.sum(before.astype(f32), axis=0, keepdims=True)
    own = mine(held_ref[...])
    chosen = own == iota((devices, blocks), 1) + 1.0
    at = jnp.sum(jnp.where(chosen, at, 0.0), axis=1, keepdims=True)
    read = jnp.sum(jnp.where(chosen, reads, 0.0), axis=1, keepdims=True)
    turn = (at == lane) & (own > 0.0)
    stands = mine((place_ref[...] & (CAP - 1)).astype(f32))
    spots = [-1.0 - own] + [mine(rank_ref[j]) for j in range(CAP - 1)]
    rows = []
    for j in range(CAP):
        spot = jnp.zeros_like(own)
        for p in range(CAP):
            spot = jnp.where(stands == float(p), spots[p ^ j], spot)
        rows.append(jnp.sum(jnp.where(turn, spot, 0.0), axis=0, keepdims=True))
    rows.append(jnp.sum(jnp.where(turn, own - 1.0, 0.0), axis=0, keepdims=True))
    by_read = jnp.sum(jnp.where(turn, read, 0.0), axis=0, keepdims=True)
    rows.append(jnp.where(iota((1, devices), 1) < blocks, by_read, float(RB_DEV)))
    rows += [jnp.zeros((1, devices), f32)] * 2
    plan_ref[...] = jnp.concatenate(rows, axis=0).astype(jnp.int32)


def lists(held_rows, blocks):
    devices = held_rows.shape[0]
    whole = pl.BlockSpec(memory_space=pltpu.VMEM)
    small = pl.BlockSpec(memory_space=pltpu.SMEM)
    square = (devices, devices)
    return pl.pallas_call(
        lists_kernel,
        grid=(1,),
        in_specs=[pl.BlockSpec((devices, NOTES, devices), lambda i: (0, blocks // NOTES, 0))],
        out_specs=(whole, small, whole, whole, whole),
        out_shape=(
            jax.ShapeDtypeStruct(((CAP - 1) * blocks, 1, devices), jnp.int32),
            jax.ShapeDtypeStruct((1,), jnp.int32),
            jax.ShapeDtypeStruct(square, jnp.float32),
            jax.ShapeDtypeStruct(square, jnp.int32),
            jax.ShapeDtypeStruct((CAP - 1,) + square, jnp.float32),
        ),
        scratch_shapes=[
            pltpu.VMEM((devices * NOTES, devices), jnp.float32),
            pltpu.VMEM((CAP - 1,) + square, jnp.float32),
        ],
        name="lists",
    )(held_rows)


def planned(me, read, held, place, ranks):
    whole = pl.BlockSpec(memory_space=pltpu.VMEM)
    return pl.pallas_call(
        plan_kernel,
        in_specs=[pl.BlockSpec(memory_space=pltpu.SMEM)] + [whole] * 4,
        out_specs=whole,
        out_shape=jax.ShapeDtypeStruct((8, held.shape[0]), jnp.int32),
        name="plan",
    )(me, read, held, place, ranks)


def pick_kernel(list_ref, rows_ref, out_ref, wide_ref, stage_ref, spare_ref, list_sem, *asked):
    group, room, lanes = out_ref.shape
    pairs = stage_ref.shape[0]

    @pl.when(pl.program_id(0) == 0)
    def _():
        copies = [
            pltpu.make_async_copy(list_ref.at[t], asked[t], list_sem) for t in range(room)
        ]
        for copy in copies:
            copy.start()
        wide_ref[...] = rows_ref[...].astype(jnp.float32)
        pltpu.make_async_copy(list_ref.at[pl.ds(0, room)], spare_ref, list_sem).wait()

    first = pl.program_id(0) * group

    def pick(i, carry):
        for u in range(pairs):
            at = i * pairs + u
            s = first + at
            for t in range(room):
                stage_ref[u, pl.ds(t, 1), :] = wide_ref[pl.ds(asked[t][0, s], 1), :]
            out_ref[at] = stage_ref[u].astype(out_ref.dtype)
        return carry

    lax.fori_loop(0, group // pairs, pick, 0)


def pick_rows(listed, rows, room):
    total, lanes = rows.shape
    devices, group, pairs = listed.shape[2], 16, 2
    return pl.pallas_call(
        pick_kernel,
        grid=(devices // group,),
        in_specs=[
            pl.BlockSpec(memory_space=pltpu.VMEM),
            pl.BlockSpec(memory_space=pltpu.VMEM),
        ],
        out_specs=pl.BlockSpec((group, room, lanes), lambda i: (i, 0, 0)),
        out_shape=jax.ShapeDtypeStruct((devices, room, lanes), rows.dtype),
        scratch_shapes=[
            pltpu.VMEM((total, lanes), jnp.float32),
            pltpu.VMEM((pairs, room, lanes), jnp.float32),
            pltpu.SMEM((room, 1, devices), jnp.int32),
            pltpu.SemaphoreType.DMA,
        ]
        + [pltpu.SMEM((1, devices), jnp.int32)] * room,
        name="pick_rows",
    )(listed, rows)


def margin_kernel(plan_ref, own_ref, got_ref, out_ref, in_ref, wide_ref, block_ref, sum_ref, other_ref, in_sem, out_sem):
    rows, room, lanes = got_ref.shape
    blocks = own_ref.shape[0]
    f32, bf16 = jnp.float32, jnp.bfloat16
    chunks = room // CHUNK
    apart = CHUNK + 1

    def fetch(c):
        return pltpu.make_async_copy(
            got_ref.at[:, pl.ds(pl.multiple_of(c * CHUNK, CHUNK), CHUNK), :], in_ref.at[c], in_sem.at[c]
        )

    for c in range(chunks):
        fetch(c).start()
    sum_ref[...] = jnp.zeros(sum_ref.shape, f32)
    other_ref[...] = jnp.zeros(other_ref.shape, f32)
    block_ref[room] = jnp.zeros((rows, lanes), bf16)

    def keep(b, carry):
        block_ref[room + 1 + b] = own_ref[b]
        return carry

    lax.fori_loop(0, blocks, keep, 0, unroll=8)

    def turn(c, carry):
        fetch(c).wait()

        def widen(d, carry):
            wide_ref[pl.ds(d * apart, CHUNK), :] = in_ref[c, d].astype(f32)
            return carry

        lax.fori_loop(0, rows, widen, 0, unroll=16)
        for t in range(CHUNK):
            block_ref[c * CHUNK + t] = wide_ref[pl.ds(t, rows, stride=apart), :].astype(bf16)
        return carry

    lax.fori_loop(0, chunks, turn, 0)

    def tiles(i):
        own = own_ref[plan_ref[CAP, i]]
        spots = [plan_ref[j, i] for j in range(CAP)]
        spots = [jnp.where(spot < 0, room - 1 - spot, spot) for spot in spots]
        for j in range(0, CAP, 2):
            pair = jnp.concatenate([block_ref[spots[j]], block_ref[spots[j + 1]]], axis=0)
            tile = lax.dot_general(own, pair, (((1,), (1,)), ((), ())), preferred_element_type=f32)
            yield tile.astype(bf16).astype(f32)

    sums = (sum_ref, other_ref)
    unroll = 16

    def leave(r, carry):
        part = pl.ds(pl.multiple_of(r * rows, rows), rows)
        sum_ref[part] += other_ref[part]
        pltpu.make_async_copy(sum_ref.at[part], out_ref.at[part], out_sem).start()
        return carry

    def step(q, carry):
        for u in range(unroll):
            i = q * unroll + u
            part = pl.ds(pl.multiple_of(plan_ref[CAP + 1, i] * rows, rows), rows)
            for j, tile in enumerate(tiles(i)):
                sums[u % 2][part, 2 * j * rows : 2 * (j + 1) * rows] += tile
        start = jnp.where(q == 0, 0, plan_ref[CAP + 1, q * unroll])
        lax.fori_loop(start, plan_ref[CAP + 1, (q + 1) * unroll], leave, 0)
        return carry

    lax.fori_loop(0, blocks // unroll, step, 0)
    pltpu.make_async_copy(sum_ref, out_ref, out_sem).wait()


def margins(plan, own, got):
    rows, room, lanes = got.shape
    blocks = own.shape[0]
    return pl.pallas_call(
        margin_kernel,
        in_specs=[
            pl.BlockSpec(memory_space=pltpu.SMEM),
            pl.BlockSpec(memory_space=pltpu.VMEM),
            pl.BlockSpec(memory_space=pl.ANY),
        ],
        out_specs=pl.BlockSpec(memory_space=pl.ANY),
        out_shape=jax.ShapeDtypeStruct((RB_DEV * rows, CAP * rows), jnp.float32),
        scratch_shapes=[
            pltpu.VMEM((room // CHUNK, rows, CHUNK, lanes), got.dtype),
            pltpu.VMEM((rows * (CHUNK + 1), lanes), jnp.float32),
            pltpu.VMEM((room + 1 + blocks, rows, lanes), own.dtype),
            pltpu.VMEM((RB_DEV * rows, CAP * rows), jnp.float32),
            pltpu.VMEM((RB_DEV * rows, CAP * rows), jnp.float32),
            pltpu.SemaphoreType.DMA((room // CHUNK,)),
            pltpu.SemaphoreType.DMA,
        ],
        name="margins",
    )(plan, own, got)


def exchange(array):
    return lax.all_to_all(array, "dev", split_axis=0, concat_axis=0, tiled=True)


def shards(occurrence, block_owner, read_block, slot_order):
    devices = lax.axis_size("dev")
    blocks, rows, kmers = occurrence.shape
    owner, read = block_owner.reshape(1, blocks), read_block.reshape(1, blocks)
    me = lax.axis_index("dev").astype(jnp.int32).reshape(1)
    held_rows = exchange(spread(slot_order, owner, occurrence))
    listed, branch, held, place, ranks = lists(held_rows, blocks)
    held_rows = held_rows.reshape(devices * (blocks + NOTES), kmers)

    def finish(room):
        outgoing = pick_rows(listed, held_rows, room)
        plan = planned(me, read, held, place, ranks)
        return margins(plan, occurrence, exchange(outgoing))

    rooms = ROOMS + ((CAP - 1) * blocks,)
    return lax.switch(branch[0], [lambda room=room: finish(room) for room in rooms])


def solution(mesh):
    placed = (P("dev", None, None), P("dev", None), P("dev"), P("dev", None))
    return jax.shard_map(
        shards, mesh=mesh, in_specs=placed, out_specs=P("dev", None), check_vma=False
    )
```
